32 devices in a mesh: tm: 8 (over z, core), dp: 4 (over y, x).
Axes of the slice: x: 2, y: 2, z: 4, core: 2. Of those that a mesh axis runs over, the one named last changes fastest.
Arguments:
- encoded: bfloat16 [512, 80, 1024], P('dp', 'tm'), may hold values from -6 to 6
- queries: bfloat16 [512, 32, 1024], P(('dp', 'tm')), may hold values from -200 to 200
- cotangent: bfloat16 [512, 32, 1024], P(('dp', 'tm')), may hold values from -0.08886719 to 0.08886719
- lengths: int32 [512], P(('dp', 'tm')), may hold values from 2 to 80
- key_weight: bfloat16 [1024, 1024], replicated, may hold values from -0.1875 to 0.1875
- value_weight: bfloat16 [1024, 1024], replicated, may hold values from -0.1875 to 0.1875
Outputs:
- context: bfloat16 [512, 32, 1024], P(('dp', 'tm'))
- key_grad: float32 [1024, 1024], replicated
- value_grad: float32 [1024, 1024], replicated
The draws below stay inside these ranges and needn't reach their ends.
Inputs may be any that keep to these rules, and one draw needn't show every extreme that they name: Sequence b attends only to source positions below lengths[b].
All inputs are finite; a program needn't handle non-finite values.
Results may differ from the reference program's by a relative error of at most 0.0069.
Values may be sent and summed in bfloat16 or wider, within the bound.
A program may use at most 128 MiB of HBM per device.

```python
import math
import jax
import jax.numpy as jnp
from jax import lax

D = 1024
SRC = 80
TGT = 32
SEQ_DEV = 16
BATCH = 512
N_DP = 4


def encoded_values(key):
    base = jax.random.fold_in(key, 11)
    drawn = jax.random.truncated_normal(base, -6.0, 6.0, (BATCH, SRC, D), jnp.float32)
    return drawn.astype(jnp.bfloat16)


def key_matrix(key):
    base = jax.random.fold_in(key, 12)
    drawn = jax.random.truncated_normal(base, -6.0, 6.0, (D, D), jnp.float32) / math.sqrt(D)
    return drawn.astype(jnp.bfloat16)


def draw_encoded(key, part):
    return encoded_values(key)


def draw_key_weight(key, part):
    return key_matrix(key)


def draw_queries(key, part):
    base = jax.random.fold_in(key, 13)
    drawn = jax.random.truncated_normal(base, -6.0, 6.0, (BATCH, TGT, D), jnp.float32)
    return drawn.astype(jnp.bfloat16)


def place_ends(result, rng, least, high):
    shape = result.shape
    spot = [jax.random.randint(jax.random.fold_in(rng, axis), (), 0, shape[axis]) for axis in range(len(shape))]
    result = result.at[tuple(spot)].set(least)
    longest = shape.index(max(shape))
    spot[longest] = (spot[longest] + 1) % shape[longest]
    return result.at[tuple(spot)].set(high)


def level_of(rng, extent, shards, smallest, high):
    def one(position, blocks):
        heights = jax.random.uniform(jax.random.fold_in(jax.random.fold_in(rng, 6), position), (blocks,), jnp.float32, smallest / len(shards), high / len(shards))
        return jnp.repeat(jnp.exp(heights), extent[position] // blocks).reshape((-1,) + (1,) * (len(extent) - position - 1))

    gain = one(*shards[0])
    for cut in shards[1:]:
        gain = gain * one(*cut)
    return gain


def normal_values(stream_key, shape, deviation, bound, split=(), kind=jnp.bfloat16):
    entries = jax.random.normal(stream_key, shape, jnp.float32) * deviation
    if len(split) > 0:
        entries = level_of(stream_key, shape, split, -0.22, 0.18) * entries
    return jnp.clip(entries, min=-bound, max=bound).astype(kind)


def setup_inputs(seed: int = 0) -> dict:
    seeds = jax.random.split(jax.random.key(seed), 7)
    encoded = draw_encoded(jax.random.fold_in(seeds[6], 71), 0)
    queries = draw_queries(jax.random.fold_in(seeds[6], 71), 0)
    cotangent = normal_values(seeds[2], (BATCH, TGT, D), (3.0 / (BATCH * SRC) ** 0.5), 0.08886719, ((0, 32),))
    lengths = place_ends(jax.random.randint(seeds[3], (BATCH,), 2, SRC + 1), jax.random.fold_in(seeds[3], 1), 2, SRC).astype(jnp.int32)
    key_weight = draw_key_weight(jax.random.fold_in(seeds[6], 71), 0)
    value_weight = normal_values(seeds[5], (D, D), D ** -0.5, 0.1875)
    return dict(encoded=encoded, queries=queries, cotangent=cotangent, lengths=lengths, key_weight=key_weight, value_weight=value_weight)


def attend(queries, key_rows, value_rows, lengths, cotangent):
    score_scale = 1.0 / math.sqrt(queries.shape[-1])
    scores = jnp.einsum('btd,bsd->bts', queries.astype(jnp.float32), key_rows.astype(jnp.float32)) * score_scale
    positions = jnp.arange(key_rows.shape[1], dtype=jnp.int32)
    in_range = positions[None, None, :] < lengths[:, None, None]
    scores = jnp.where(in_range, scores, -1e+30)
    row_max = lax.optimization_barrier(jnp.max(scores, axis=-1, keepdims=True))
    weights = jnp.exp(scores - row_max)
    probabilities = weights / lax.optimization_barrier(jnp.sum(weights, axis=-1, keepdims=True))
    probs_low = lax.optimization_barrier(probabilities.astype(jnp.bfloat16))
    context = jnp.einsum('bts,bsd->btd', probs_low.astype(jnp.float32), value_rows.astype(jnp.float32)).astype(jnp.bfloat16)
    grad_probs = jnp.einsum('btd,bsd->bts', cotangent.astype(jnp.float32), value_rows.astype(jnp.float32))
    grad_scores = probabilities * (grad_probs - lax.optimization_barrier(jnp.sum(probabilities * grad_probs, axis=-1, keepdims=True)))
    grad_low = lax.optimization_barrier(grad_scores.astype(jnp.bfloat16))
    grad_values = jnp.einsum('bts,btd->bsd', probs_low.astype(jnp.float32), cotangent.astype(jnp.float32)).astype(jnp.bfloat16)
    grad_keys = (jnp.einsum('bts,btd->bsd', grad_low.astype(jnp.float32), queries.astype(jnp.float32)) * score_scale).astype(jnp.bfloat16)
    return (context, grad_keys, grad_values)

def reference(encoded, queries, cotangent, lengths, key_weight, value_weight):
    block_rows = SEQ_DEV * N_DP
    block_count = BATCH // block_rows
    enc_blocks = encoded.reshape(block_count, block_rows, SRC, D)
    query_blocks = queries.reshape(block_count, block_rows, TGT, D)
    cotan_blocks = cotangent.reshape(block_count, block_rows, TGT, D)
    length_blocks = lengths.reshape(block_count, block_rows)

    def scan_step(totals, pieces):
        enc_block, query_block, cotan_block, length_block = pieces
        flattened = enc_block.reshape(-1, D)
        key_rows = jnp.dot(flattened, key_weight, preferred_element_type=jnp.float32).astype(jnp.bfloat16).reshape(block_rows, SRC, D)
        value_rows = jnp.dot(flattened, value_weight, preferred_element_type=jnp.float32).astype(jnp.bfloat16).reshape(block_rows, SRC, D)
        context, grad_keys, grad_values = attend(query_block, key_rows, value_rows, length_block, cotan_block)
        key_total = totals[0] + jnp.dot(flattened.T, grad_keys.reshape(-1, D), preferred_element_type=jnp.float32)
        value_total = totals[1] + jnp.dot(flattened.T, grad_values.reshape(-1, D), preferred_element_type=jnp.float32)
        return ((key_total, value_total), context)
    zeros = jnp.zeros((D, D), jnp.float32)
    totals, contexts = lax.scan(scan_step, (zeros, zeros), (enc_blocks, query_blocks, cotan_blocks, length_blocks))
    return (contexts.reshape(BATCH, TGT, D), totals[0], totals[1])
```

```python
import functools
import math

import jax
import jax.numpy as jnp
from jax import lax
from jax.experimental import pallas as pl
from jax.experimental.pallas import tpu as pltpu
from jax.sharding import PartitionSpec as P

MESH = pl.DeviceIdType.MESH


def bit_of(index, k):
    return lax.rem(index // (1 << k), 2)


def flip(index, mask):
    k = 0
    while (1 << k) <= mask:
        if mask & (1 << k):
            index = index + (1 - 2 * bit_of(index, k)) * (1 << k)
        k += 1
    return index


def greet(devices):
    barrier = pltpu.get_barrier_semaphore()
    for device in devices:
        pl.semaphore_signal(barrier, inc=1, device_id=device, device_id_type=MESH)
    pl.semaphore_wait(barrier, len(devices))


def exchange_kernel(n, enc_ref, out_ref, send_sem, recv_sem, own_sem):
    me = lax.axis_index("tm")
    seqs = out_ref.shape[2]
    greet([{"tm": flip(me, d)} for d in range(1, n)])
    copies = []
    for d in range(n - 1, 0, -1):
        target = flip(me, d)
        copy = pltpu.make_async_remote_copy(
            src_ref=enc_ref.at[:, pl.ds(pl.multiple_of(target * seqs, seqs), seqs), :],
            dst_ref=out_ref.at[me],
            send_sem=send_sem.at[d],
            recv_sem=recv_sem.at[d],
            device_id={"tm": target},
            device_id_type=MESH,
        )
        copy.start()
        copies.append(copy)
    own = pltpu.make_async_copy(
        enc_ref.at[:, pl.ds(pl.multiple_of(me * seqs, seqs), seqs), :], out_ref.at[me], own_sem
    )
    own.start()
    own.wait()
    for copy in copies:
        copy.wait()


def exchange(encoded, n):
    by_position = jnp.swapaxes(encoded, 0, 1)
    positions, rows, width = by_position.shape
    return pl.pallas_call(
        functools.partial(exchange_kernel, n),
        out_shape=jax.ShapeDtypeStruct((n, positions, rows // n, width), encoded.dtype),
        in_specs=[pl.BlockSpec(memory_space=pltpu.VMEM)],
        out_specs=pl.BlockSpec(memory_space=pltpu.VMEM),
        scratch_shapes=[
            pltpu.SemaphoreType.DMA((n,)),
            pltpu.SemaphoreType.DMA((n,)),
            pltpu.SemaphoreType.DMA,
        ],
        compiler_params=pltpu.CompilerParams(
            collective_id=0, has_side_effects=True, vmem_limit_bytes=40 << 20
        ),
    )(by_position)


def orders_of(bits_tm, bits_dp):
    middle = [("dp", k) for k in range(bits_dp)] + [("tm", k) for k in range(1, bits_tm - 1)]
    last = [("tm", bits_tm - 1)] if bits_tm > 1 else []
    return [middle[p:] + middle[:p] + last for p in range(3)]


def partner_of(position, step):
    axis, k = step
    return {axis: flip(position[axis], 1 << k)}


def sum_kernel(bits, key_ref, value_ref, out_ref, held, staged, landed, send_sem, recv_sem):
    position = {"tm": lax.axis_index("tm"), "dp": lax.axis_index("dp")}
    rows, width = key_ref.shape
    orders = orders_of(*bits)
    tiles = width // 128
    edges = [0, (tiles * 3 // 8) * 128, (tiles * 6 // 8) * 128, width]
    greet(
        [partner_of(position, ("tm", k)) for k in range(bits[0])]
        + [partner_of(position, ("dp", k)) for k in range(bits[1])]
    )
    core = bit_of(position["tm"], 0)
    chunk = 64

    def each(start, size, body):
        piece = min(chunk, size)

        @pl.loop(0, size // piece)
        def _(i):
            body(pl.ds(pl.multiple_of(start + i * piece, piece), piece), i * piece, piece)

    def send(src, dst, slot, device):
        copy = pltpu.make_async_remote_copy(
            src_ref=src,
            dst_ref=dst,
            send_sem=send_sem.at[slot],
            recv_sem=recv_sem.at[slot],
            device_id=device,
            device_id_type=MESH,
        )
        copy.start()
        return copy

    def stage_core(ref):
        def body(at, _, __):
            staged[at, :] = ref[at, :].astype(staged.dtype)

        each(0, rows, body)

    @pl.when(core == 0)
    def _():
        stage_core(value_ref)

    @pl.when(core == 1)
    def _():
        stage_core(key_ref)

    first = send(staged.at[pl.ds(0, rows)], landed.at[pl.ds(0, rows)], 0, partner_of(position, ("tm", 0)))
    first.wait()

    def add_core(ref):
        def body(at, _, __):
            held[at, :] = ref[at, :] + landed[at, :].astype(jnp.float32)

        each(0, rows, body)

    @pl.when(core == 0)
    def _():
        add_core(key_ref)

    @pl.when(core == 1)
    def _():
        add_core(value_ref)

    steps = len(orders[0])
    begin = [jnp.int32(0) for _ in orders]
    size = rows
    base = rows
    starts = [list(begin)]
    for step in range(steps):
        size //= 2
        copies = []
        for p, order in enumerate(orders):
            axis, k = order[step]
            bit = bit_of(position[axis], k)
            cols = pl.ds(edges[p], edges[p + 1] - edges[p])
            away = begin[p] + (1 - bit) * size
            begin[p] = begin[p] + bit * size

            def body(at, i, piece, cols=cols):
                staged[pl.ds(pl.multiple_of(base + i, piece), piece), cols] = held[at, cols].astype(
                    staged.dtype
                )

            each(away, size, body)
            copies.append(
                send(
                    staged.at[pl.ds(base, size), cols],
                    landed.at[pl.ds(base, size), cols],
                    1 + step * 3 + p,
                    partner_of(position, order[step]),
                )
            )
        for p, copy in enumerate(copies):
            copy.wait()
            cols = pl.ds(edges[p], edges[p + 1] - edges[p])

            def body(at, i, piece, cols=cols):
                held[at, cols] += landed[pl.ds(pl.multiple_of(base + i, piece), piece), cols].astype(
                    jnp.float32
                )

            each(begin[p], size, body)
        starts.append(list(begin))
        base += size

    for p in range(3):
        cols = pl.ds(edges[p], edges[p + 1] - edges[p])

        def body(at, i, piece, cols=cols, p=p):
            out_ref[
                pl.ds(pl.multiple_of(core * rows + begin[p] + i, piece), piece), cols
            ] = held[at, cols].astype(out_ref.dtype)

        each(begin[p], size, body)

    slot = 1 + steps * 3
    for step in range(steps - 1, -1, -1):
        copies = []
        for p, order in enumerate(orders):
            at = (
                pl.ds(pl.multiple_of(core * rows + starts[step + 1][p], size), size),
                pl.ds(edges[p], edges[p + 1] - edges[p]),
            )
            copies.append(
                send(out_ref.at[at], out_ref.at[at], slot + step * 3 + p, partner_of(position, order[step]))
            )
        for copy in copies:
            copy.wait()
        size *= 2
    at = pl.ds(pl.multiple_of(core * rows, rows), rows)
    send(out_ref.at[at], out_ref.at[at], slot + steps * 3, partner_of(position, ("tm", 0))).wait()


def sum_everywhere(key_term, value_term, bits):
    rows, width = key_term.shape
    slots = 2 + 6 * (bits[0] + bits[1] - 1)
    return pl.pallas_call(
        functools.partial(sum_kernel, bits),
        out_shape=jax.ShapeDtypeStruct((2 * rows, width), jnp.bfloat16),
        in_specs=[pl.BlockSpec(memory_space=pltpu.VMEM)] * 2,
        out_specs=pl.BlockSpec(memory_space=pltpu.VMEM),
        scratch_shapes=[
            pltpu.VMEM((rows, width), jnp.float32),
            pltpu.VMEM((2 * rows, width), jnp.bfloat16),
            pltpu.VMEM((2 * rows, width), jnp.bfloat16),
            pltpu.SemaphoreType.DMA((slots,)),
            pltpu.SemaphoreType.DMA((slots,)),
        ],
        compiler_params=pltpu.CompilerParams(
            collective_id=1, has_side_effects=True, vmem_limit_bytes=48 << 20
        ),
    )(key_term, value_term)


def attend(queries, keys, values, lengths, cotangent, seqs):
    score_scale = 1.0 / math.sqrt(queries.shape[-1])
    steps = queries.shape[0] // seqs
    dot = functools.partial(lax.dot_general, preferred_element_type=jnp.float32)
    rows_rows = (((1,), (1,)), ((), ()))
    rows_cols = (((1,), (0,)), ((), ()))
    cols_cols = (((0,), (0,)), ((), ()))
    scores = dot(queries, keys, rows_rows) * score_scale
    row = lax.broadcasted_iota(jnp.int32, (queries.shape[0], 1), 0) // steps
    column = lax.broadcasted_iota(jnp.int32, (1, keys.shape[0]), 1)
    limit = jnp.repeat(lengths, steps)[:, None]
    seen = (column % seqs == row) & (column // seqs < limit)
    scores = jnp.where(seen, scores, -1e30)
    row_max = jnp.max(scores, axis=-1, keepdims=True)
    weights = jnp.where(seen, jnp.exp(scores - row_max), 0.0)
    probabilities = weights / jnp.sum(weights, axis=-1, keepdims=True)
    probs_low = probabilities.astype(jnp.bfloat16)
    context = dot(probs_low, values, rows_cols).astype(jnp.bfloat16)
    grad_probs = dot(cotangent, values, rows_rows)
    grad_scores = probabilities * (
        grad_probs - jnp.sum(probabilities * grad_probs, axis=-1, keepdims=True)
    )
    grad_low = grad_scores.astype(jnp.bfloat16)
    grad_values = dot(probs_low, cotangent, cols_cols).astype(jnp.bfloat16)
    grad_keys = (dot(grad_low, queries, cols_cols) * score_scale).astype(jnp.bfloat16)
    return context, grad_keys, grad_values


def project(flattened, weight_matrix):
    return jnp.dot(flattened, weight_matrix, preferred_element_type=jnp.float32).astype(jnp.bfloat16)


def weight_term(flattened, gradient):
    return lax.dot_general(
        flattened, gradient, (((0,), (0,)), ((), ())), preferred_element_type=jnp.float32
    )


def body(n_tm, n_dp, encoded, queries, cotangent, lengths, key_weight, value_weight):
    width = encoded.shape[2]
    seqs = queries.shape[0]
    flattened = exchange(encoded, n_tm).reshape(-1, width)
    key_rows = project(flattened, key_weight)
    value_rows = project(flattened, value_weight)
    context, grad_keys, grad_values = attend(
        queries.reshape(-1, width), key_rows, value_rows, lengths, cotangent.reshape(-1, width), seqs
    )
    key_term = weight_term(flattened, grad_keys)
    value_term = weight_term(flattened, grad_values)
    sums = sum_everywhere(
        key_term, value_term, (n_tm.bit_length() - 1, n_dp.bit_length() - 1)
    ).astype(jnp.float32)
    return context.reshape(queries.shape), sums[: key_term.shape[0]], sums[key_term.shape[0] :]


def solution(mesh):
    return jax.shard_map(
        functools.partial(body, mesh.shape["tm"], mesh.shape["dp"]),
        mesh=mesh,
        in_specs=(
            P("dp", "tm", None),
            P(("dp", "tm"), None, None),
            P(("dp", "tm"), None, None),
            P(("dp", "tm")),
            P(),
            P(),
        ),
        out_specs=(P(("dp", "tm"), None, None), P(), P()),
        check_vma=False,
    )
```

```python
import functools
import math

import jax
import jax.numpy as jnp
from jax import lax
from jax.experimental import pallas as pl
from jax.experimental.pallas import tpu as pltpu
from jax.sharding import PartitionSpec as P

MESH = pl.DeviceIdType.MESH


def bit_of(index, k):
    return lax.rem(index // (1 << k), 2)


def flip(index, mask):
    k = 0
    while (1 << k) <= mask:
        if mask & (1 << k):
            index = index + (1 - 2 * bit_of(index, k)) * (1 << k)
        k += 1
    return index


def greet(devices):
    barrier = pltpu.get_barrier_semaphore()
    for device in devices:
        pl.semaphore_signal(barrier, inc=1, device_id=device, device_id_type=MESH)
    pl.semaphore_wait(barrier, len(devices))


def exchange_kernel(n, enc_ref, kw_ref, vw_ref, out_ref, key_ref, value_ref, send_sem, recv_sem, own_sem):
    me = lax.axis_index("tm")
    _, positions, seqs, width = out_ref.shape
    greet([{"tm": flip(me, d)} for d in range(1, n)])
    copies = {}
    for d in range(n - 1, 0, -1):
        target = flip(me, d)
        copies[d] = pltpu.make_async_remote_copy(
            src_ref=enc_ref.at[:, pl.ds(pl.multiple_of(target * seqs, seqs), seqs), :],
            dst_ref=out_ref.at[me],
            send_sem=send_sem.at[d],
            recv_sem=recv_sem.at[d],
            device_id={"tm": target},
            device_id_type=MESH,
        )
        copies[d].start()
    own = pltpu.make_async_copy(
        enc_ref.at[:, pl.ds(pl.multiple_of(me * seqs, seqs), seqs), :], out_ref.at[me], own_sem
    )
    own.start()
    own.wait()

    def project(source):
        block = out_ref[source].reshape(positions * seqs, width)
        for weight, rows in ((kw_ref, key_ref), (vw_ref, value_ref)):
            rows[source] = jnp.dot(
                block, weight[...], preferred_element_type=jnp.float32
            ).astype(rows.dtype)

    project(me)
    for d in [1] + list(range(n - 1, 1, -1)):
        copies[d].wait()
        project(flip(me, d))


def exchange(encoded, key_weight, value_weight, n):
    by_position = jnp.swapaxes(encoded, 0, 1)
    positions, rows, width = by_position.shape
    taken = (n, positions, rows // n, width)
    projected = (n, positions * rows // n, width)
    results = pl.pallas_call(
        functools.partial(exchange_kernel, n),
        out_shape=[
            jax.ShapeDtypeStruct(taken, encoded.dtype),
            jax.ShapeDtypeStruct(projected, encoded.dtype),
            jax.ShapeDtypeStruct(projected, encoded.dtype),
        ],
        in_specs=[pl.BlockSpec(memory_space=pltpu.VMEM)] * 3,
        out_specs=[pl.BlockSpec(memory_space=pltpu.VMEM)] * 3,
        scratch_shapes=[
            pltpu.SemaphoreType.DMA((n,)),
            pltpu.SemaphoreType.DMA((n,)),
            pltpu.SemaphoreType.DMA,
        ],
        compiler_params=pltpu.CompilerParams(
            collective_id=0, has_side_effects=True, vmem_limit_bytes=48 << 20
        ),
    )(by_position, key_weight, value_weight)
    return [result.reshape(-1, width) for result in results]


def orders_of(bits_tm, bits_dp):
    middle = [("dp", k) for k in range(bits_dp)] + [("tm", k) for k in range(1, bits_tm - 1)]
    last = [("tm", bits_tm - 1)] if bits_tm > 1 else []
    return [middle[p:] + middle[:p] + last for p in range(3)]


def partner_of(position, step):
    axis, k = step
    return {axis: flip(position[axis], 1 << k)}


def sum_kernel(bits, key_ref, value_ref, out_ref, held, staged, landed, send_sem, recv_sem):
    position = {"tm": lax.axis_index("tm"), "dp": lax.axis_index("dp")}
    rows, width = key_ref.shape
    orders = orders_of(*bits)
    tiles = width // 128
    edges = [0, (tiles * 3 // 8) * 128, (tiles * 6 // 8) * 128, width]
    greet(
        [partner_of(position, ("tm", k)) for k in range(bits[0])]
        + [partner_of(position, ("dp", k)) for k in range(bits[1])]
    )
    core = bit_of(position["tm"], 0)
    chunk = 64

    def each(start, size, body):
        piece = min(chunk, size)

        @pl.loop(0, size // piece)
        def _(i):
            body(pl.ds(pl.multiple_of(start + i * piece, piece), piece), i * piece, piece)

    def send(src, dst, slot, device):
        copy = pltpu.make_async_remote_copy(
            src_ref=src,
            dst_ref=dst,
            send_sem=send_sem.at[slot],
            recv_sem=recv_sem.at[slot],
            device_id=device,
            device_id_type=MESH,
        )
        copy.start()
        return copy

    def stage_core(ref):
        def body(at, _, __):
            staged[at, :] = ref[at, :].astype(staged.dtype)

        each(0, rows, body)

    @pl.when(core == 0)
    def _():
        stage_core(value_ref)

    @pl.when(core == 1)
    def _():
        stage_core(key_ref)

    first = send(staged.at[pl.ds(0, rows)], landed.at[pl.ds(0, rows)], 0, partner_of(position, ("tm", 0)))
    first.wait()

    def add_core(ref):
        def body(at, _, __):
            held[at, :] = ref[at, :] + landed[at, :].astype(jnp.float32)

        each(0, rows, body)

    @pl.when(core == 0)
    def _():
        add_core(key_ref)

    @pl.when(core == 1)
    def _():
        add_core(value_ref)

    steps = len(orders[0])
    begin = [jnp.int32(0) for _ in orders]
    size = rows
    base = rows
    starts = [list(begin)]
    for step in range(steps):
        size //= 2
        copies = []
        for p, order in enumerate(orders):
            axis, k = order[step]
            bit = bit_of(position[axis], k)
            cols = pl.ds(edges[p], edges[p + 1] - edges[p])
            away = begin[p] + (1 - bit) * size
            begin[p] = begin[p] + bit * size

            def body(at, i, piece, cols=cols):
                staged[pl.ds(pl.multiple_of(base + i, piece), piece), cols] = held[at, cols].astype(
                    staged.dtype
                )

            each(away, size, body)
            copies.append(
                send(
                    staged.at[pl.ds(base, size), cols],
                    landed.at[pl.ds(base, size), cols],
                    1 + step * 3 + p,
                    partner_of(position, order[step]),
                )
            )
        for p, copy in enumerate(copies):
            copy.wait()
            cols = pl.ds(edges[p], edges[p + 1] - edges[p])

            def body(at, i, piece, cols=cols):
                held[at, cols] += landed[pl.ds(pl.multiple_of(base + i, piece), piece), cols].astype(
                    jnp.float32
                )

            each(begin[p], size, body)
        starts.append(list(begin))
        base += size

    for p in range(3):
        cols = pl.ds(edges[p], edges[p + 1] - edges[p])

        def body(at, i, piece, cols=cols, p=p):
            out_ref[
                pl.ds(pl.multiple_of(core * rows + begin[p] + i, piece), piece), cols
            ] = held[at, cols].astype(out_ref.dtype)

        each(begin[p], size, body)

    slot = 1 + steps * 3
    for step in range(steps - 1, -1, -1):
        copies = []
        for p, order in enumerate(orders):
            at = (
                pl.ds(pl.multiple_of(core * rows + starts[step + 1][p], size), size),
                pl.ds(edges[p], edges[p + 1] - edges[p]),
            )
            copies.append(
                send(out_ref.at[at], out_ref.at[at], slot + step * 3 + p, partner_of(position, order[step]))
            )
        for copy in copies:
            copy.wait()
        size *= 2
    at = pl.ds(pl.multiple_of(core * rows, rows), rows)
    send(out_ref.at[at], out_ref.at[at], slot + steps * 3, partner_of(position, ("tm", 0))).wait()


def sum_everywhere(key_term, value_term, bits):
    rows, width = key_term.shape
    slots = 2 + 6 * (bits[0] + bits[1] - 1)
    return pl.pallas_call(
        functools.partial(sum_kernel, bits),
        out_shape=jax.ShapeDtypeStruct((2 * rows, width), jnp.bfloat16),
        in_specs=[pl.BlockSpec(memory_space=pltpu.VMEM)] * 2,
        out_specs=pl.BlockSpec(memory_space=pltpu.VMEM),
        scratch_shapes=[
            pltpu.VMEM((rows, width), jnp.float32),
            pltpu.VMEM((2 * rows, width), jnp.bfloat16),
            pltpu.VMEM((2 * rows, width), jnp.bfloat16),
            pltpu.SemaphoreType.DMA((slots,)),
            pltpu.SemaphoreType.DMA((slots,)),
        ],
        compiler_params=pltpu.CompilerParams(
            collective_id=1, has_side_effects=True, vmem_limit_bytes=48 << 20
        ),
    )(key_term, value_term)


def attend(queries, keys, values, lengths, cotangent, seqs):
    score_scale = 1.0 / math.sqrt(queries.shape[-1])
    steps = queries.shape[0] // seqs
    dot = functools.partial(lax.dot_general, preferred_element_type=jnp.float32)
    rows_rows = (((1,), (1,)), ((), ()))
    rows_cols = (((1,), (0,)), ((), ()))
    cols_cols = (((0,), (0,)), ((), ()))
    scores = dot(queries, keys, rows_rows) * score_scale
    row = lax.broadcasted_iota(jnp.int32, (queries.shape[0], 1), 0) // steps
    column = lax.broadcasted_iota(jnp.int32, (1, keys.shape[0]), 1)
    limit = jnp.repeat(lengths, steps)[:, None]
    seen = (column % seqs == row) & (column // seqs < limit)
    scores = jnp.where(seen, scores, -1e30)
    row_max = jnp.max(scores, axis=-1, keepdims=True)
    weights = jnp.where(seen, jnp.exp(scores - row_max), 0.0)
    probabilities = weights / jnp.sum(weights, axis=-1, keepdims=True)
    probs_low = probabilities.astype(jnp.bfloat16)
    context = dot(probs_low, values, rows_cols).astype(jnp.bfloat16)
    grad_probs = dot(cotangent, values, rows_rows)
    grad_scores = probabilities * (
        grad_probs - jnp.sum(probabilities * grad_probs, axis=-1, keepdims=True)
    )
    grad_low = grad_scores.astype(jnp.bfloat16)
    grad_values = dot(probs_low, cotangent, cols_cols).astype(jnp.bfloat16)
    grad_keys = (dot(grad_low, queries, cols_cols) * score_scale).astype(jnp.bfloat16)
    return context, grad_keys, grad_values


def weight_term(flattened, gradient):
    return lax.dot_general(
        flattened, gradient, (((0,), (0,)), ((), ())), preferred_element_type=jnp.float32
    )


def body(n_tm, n_dp, encoded, queries, cotangent, lengths, key_weight, value_weight):
    width = encoded.shape[2]
    seqs = queries.shape[0]
    flattened, key_rows, value_rows = exchange(encoded, key_weight, value_weight, n_tm)
    context, grad_keys, grad_values = attend(
        queries.reshape(-1, width), key_rows, value_rows, lengths, cotangent.reshape(-1, width), seqs
    )
    key_term = weight_term(flattened, grad_keys)
    value_term = weight_term(flattened, grad_values)
    sums = sum_everywhere(
        key_term, value_term, (n_tm.bit_length() - 1, n_dp.bit_length() - 1)
    ).astype(jnp.float32)
    return context.reshape(queries.shape), sums[: key_term.shape[0]], sums[key_term.shape[0] :]


def solution(mesh):
    return jax.shard_map(
        functools.partial(body, mesh.shape["tm"], mesh.shape["dp"]),
        mesh=mesh,
        in_specs=(
            P("dp", "tm", None),
            P(("dp", "tm"), None, None),
            P(("dp", "tm"), None, None),
            P(("dp", "tm")),
            P(),
            P(),
        ),
        out_specs=(P(("dp", "tm"), None, None), P(), P()),
        check_vma=False,
    )
```
